256 devices in a mesh: ma: 64 (over x, z, core), freq: 4 (over y).
Axes of the slice: x: 4, y: 4, z: 8, core: 2. Of those that a mesh axis runs over, the one named last changes fastest.
Arguments:
- visibilities: bfloat16 [128, 192, 16, 2, 512], P('ma', None, 'freq')
- eigenmodes: bfloat16 [128, 16, 2, 512, 256], P('ma', 'freq'), may hold values from -0.375 to 0.375
- retained: int32 [128], P('ma'), may hold values from 1 to 256
Outputs:
- coefficients: bfloat16 [128, 2, 192, 256], P('ma')
- filtered: bfloat16 [128, 192, 16, 2, 512], P('ma', None, 'freq')
The draws below stay inside these ranges and needn't reach their ends.
All inputs are finite; a program needn't handle non-finite values.
Results may differ from the reference program's by a relative error of at most 0.0049.
Values may be sent and summed in bfloat16 or wider, within the bound.
A program may use at most 128 MiB of HBM per device.

```python
import jax
import jax.numpy as jnp
from jax import lax

BASE = 512
KMAX = 256
SAMPLES = 192
MODES = 128
FREQS = 16


def draw_visibilities(key, part):
    shape = (MODES, SAMPLES, FREQS, 2, BASE)
    first, second = jax.random.split(key, 2)
    m_scale = 1.0 + 2.0 * jnp.arange(MODES, dtype=jnp.float32) / max(MODES - 1, 1)
    s_scale = jnp.exp(jax.random.uniform(second, (SAMPLES,), jnp.float32) * jnp.log(10.0))
    noise = jax.random.normal(first, shape, jnp.float32)
    values = noise * m_scale[:, None, None, None, None] * s_scale[None, :, None, None, None] / 3.0
    return values.astype(jnp.bfloat16)


def set_ends(result, rng, smallest, top_value):
    longest = result.shape.index(max(result.shape))
    spots = []
    for shift in (0, 1):
        where = [jax.random.randint(jax.random.fold_in(rng, axis), (), 0, length) for axis, length in enumerate(result.shape)]
        where[longest] = (where[longest] + shift) % result.shape[longest]
        spots.append(tuple(where))
    return result.at[spots[0]].set(smallest).at[spots[1]].set(top_value)


def block_scale(stream_key, shape, cuts, smallest, top_value):
    loudness = 1.0
    for dim, shards_of in cuts:
        heights = jax.random.uniform(jax.random.fold_in(jax.random.fold_in(stream_key, 6), dim), (shards_of,), jnp.float32, smallest / len(cuts), top_value / len(cuts))
        loudness = loudness * jnp.repeat(jnp.exp(heights), shape[dim] // shards_of).reshape((-1,) + (1,) * (len(shape) - 1 - dim))
    return loudness


def normal_values(key, shape, scale, most, cuts=(), kind=jnp.bfloat16):
    values = scale * jax.random.normal(key, shape, jnp.float32)
    if cuts:
        values = values * block_scale(key, shape, cuts, -0.22, 0.18)
    return jnp.clip(values, -most, most).astype(kind)


def setup_inputs(seed: int = 0) -> dict:
    key_of = jax.random.split(jax.random.key(seed), 4)
    visibilities = draw_visibilities(jax.random.fold_in(key_of[3], 71), 0)
    eigenmodes = normal_values(key_of[1], (MODES, FREQS, 2, BASE, KMAX), KMAX ** -0.5, 0.375, ((0, 64), (1, 4)))
    retained = set_ends(jax.random.randint(key_of[2], (MODES,), 1, KMAX + 1), jax.random.fold_in(key_of[2], 1), 1, KMAX).astype(jnp.int32)
    return {"visibilities": visibilities, "eigenmodes": eigenmodes, "retained": retained}


def reference(visibilities, eigenmodes, retained):
    modes_all, samples, freqs, _, base = visibilities.shape
    kmax = eigenmodes.shape[-1]
    width = freqs * 2 * base

    def project(item):
        vis, vecs = item
        flat = vis.reshape(samples, width)
        swapped = jnp.stack([vis[:, :, 1, :], -vis[:, :, 0, :]], axis=2).reshape(samples, width)
        matrix = vecs.reshape(width, kmax)
        return (jnp.dot(flat, matrix, preferred_element_type=jnp.float32), jnp.dot(swapped, matrix, preferred_element_type=jnp.float32))
    proj_re, proj_im = lax.map(project, (visibilities, eigenmodes))
    keep = (jnp.arange(kmax, dtype=jnp.int32)[None, :] < retained[:, None]).astype(jnp.float32)
    power = lax.optimization_barrier(jnp.sum(keep[:, None, :] * (proj_re * proj_re + proj_im * proj_im), axis=(0, 1)))
    count = jnp.float32(samples) * lax.optimization_barrier(jnp.sum(keep, axis=0))
    scale = 1.0 / jnp.sqrt(power / jnp.maximum(count, 1.0) + 1e-06)
    gain = keep * scale[None, :]
    coef_re = (proj_re * gain[:, None, :]).astype(jnp.bfloat16)
    coef_im = (proj_im * gain[:, None, :]).astype(jnp.bfloat16)

    def back(item):
        cre, cim, vecs = item
        matrix = vecs.reshape(width, kmax)
        first = jnp.dot(cre, matrix.T, preferred_element_type=jnp.float32).reshape(samples, freqs, 2, base)
        second = jnp.dot(cim, matrix.T, preferred_element_type=jnp.float32).reshape(samples, freqs, 2, base)
        out_re = first[:, :, 0, :] - second[:, :, 1, :]
        out_im = second[:, :, 0, :] + first[:, :, 1, :]
        return jnp.stack([out_re, out_im], axis=2).astype(jnp.bfloat16)
    filtered = lax.map(back, (coef_re, coef_im, eigenmodes))
    coefficients = jnp.stack([coef_re, coef_im], axis=1)
    return (coefficients, filtered)
```

```python
import functools

import jax
import jax.numpy as jnp
from jax import lax
from jax.experimental import pallas as pl
from jax.experimental.pallas import tpu as pltpu
from jax.sharding import PartitionSpec as P

MESH = pl.DeviceIdType.MESH
BF16, F32 = jnp.bfloat16, jnp.float32
NX, NZ, NCORE, NY = 4, 8, 2, 4
LANES = 128


def pair_turn(x, odd_sign):
    rows, cols = x.shape
    tiles = x.reshape(rows // 8, 8, cols)
    even = lax.broadcasted_iota(jnp.int32, tiles.shape, 1) % 2 == 0
    turned = jnp.where(even, -odd_sign * pltpu.roll(tiles, 7, 1), odd_sign * pltpu.roll(tiles, 1, 1))
    return turned.reshape(rows, cols)


def project_kernel(
    ret_ref, x_hbm, e_hbm, g_ref, s_ref, eb,
    xb, acc_re, acc_im, pf, sbuf, rbuf, a1, a2,
    x_sem, e_sem, rs_send, rs_recv, ag_send, ag_recv, z_send, z_recv, w_send, w_recv,
):
    modes, freqs, half = xb.shape[0], e_hbm.shape[1], rbuf.shape[1]
    blocks = xb.shape[1] // freqs
    rows, kmax = sbuf.shape[1:]
    ma = lax.axis_index("ma")
    y = lax.axis_index("freq")
    core = lax.rem(ma, NCORE)
    z = lax.rem(ma // NCORE, NZ)
    x = ma // (NCORE * NZ)

    def x_copy(m, f, b):
        j = f * blocks + b
        return pltpu.make_async_copy(
            x_hbm.at[m, :, f, :, pl.ds(b * LANES, LANES)], xb.at[m, j], x_sem.at[m, j]
        )

    def e_copy(m, f):
        return pltpu.make_async_copy(e_hbm.at[m, f], eb.at[m, f], e_sem.at[m, f])

    for m in range(modes):
        for f in range(freqs):
            e_copy(m, f).start()
            for b in range(blocks):
                x_copy(m, f, b).start()

    z_peers = [((x * NZ + lax.rem(z + d, NZ)) * NCORE + core, lax.rem(z + d, NZ)) for d in range(NZ)]
    xs = [lax.rem(x + d, NX) for d in range(NX)]
    ys = [lax.rem(y + d, NY) for d in range(NY)]
    cs = [core, 1 - core]
    far = [2, 1, 3, 0]
    w_peers = [
        ((xs[dx] * NZ + z) * NCORE + cs[dc], ys[dy])
        for dx in far for dy in far for dc in (1, 0)
        if (dx, dy, dc) != (0, 0, 0)
    ]
    barrier = pltpu.get_barrier_semaphore()
    for peer in w_peers:
        pl.semaphore_signal(barrier, inc=1, device_id={"ma": peer[0], "freq": peer[1]}, device_id_type=MESH)
    for d in range(1, NZ):
        pl.semaphore_signal(barrier, inc=1, device_id={"ma": z_peers[d][0], "freq": y}, device_id_type=MESH)

    def rs_copy(m, h):
        t = 2 * m + h
        return pltpu.make_async_remote_copy(
            src_ref=sbuf.at[m, pl.ds(h * half, half)], dst_ref=rbuf.at[y],
            send_sem=rs_send.at[t], recv_sem=rs_recv.at[y],
            device_id={"ma": ma, "freq": t}, device_id_type=MESH,
        )

    for m in range(modes):
        for f in range(freqs):
            e_copy(m, f).wait()
            for b in range(blocks):
                x_copy(m, f, b).wait()
            lhs = jnp.concatenate(
                [xb.at[m, f * blocks + b].reshape(rows, LANES)[...] for b in range(blocks)], axis=1
            )
            d_re = jnp.dot(lhs, eb[m, f, 0], preferred_element_type=F32)
            d_im = jnp.dot(lhs, eb[m, f, 1], preferred_element_type=F32)
            if f == 0:
                acc_re[...] = d_re
                acc_im[...] = d_im
            else:
                acc_re[...] += d_re
                acc_im[...] += d_im
        proj = acc_re[...] + pair_turn(acc_im[...], -1.0)
        pf[m] = proj
        sbuf[m] = proj.astype(BF16)
        if m == 0:
            pl.semaphore_wait(barrier, len(w_peers) + NZ - 1)
        for h in range(2):
            @pl.when(2 * m + h != y)
            def _():
                rs_copy(m, h).start()

    share = pf[y // 2, pl.ds(lax.rem(y, 2) * half, half), :]
    for d in range(1, NY):
        src = ys[d]
        pltpu.make_async_remote_copy(
            src_ref=sbuf.at[0, pl.ds(0, half)], dst_ref=rbuf.at[src],
            send_sem=rs_send.at[src], recv_sem=rs_recv.at[src],
            device_id={"ma": ma, "freq": src}, device_id_type=MESH,
        ).wait_recv()
        share = share + rbuf[src].astype(F32)
    cut = ret_ref[y // 2]
    keep = (lax.broadcasted_iota(jnp.int32, (1, kmax), 1) < cut).astype(F32)
    power = keep * jnp.sum(share * share, axis=0, keepdims=True)
    count = keep * (half // 2)
    parts = kmax // LANES
    for p in range(parts):
        a1[z, pl.ds(p, 1), :] = power[:, p * LANES : (p + 1) * LANES]
        a1[z, pl.ds(parts + p, 1), :] = count[:, p * LANES : (p + 1) * LANES]

    def z_copy(d):
        return pltpu.make_async_remote_copy(
            src_ref=a1.at[z], dst_ref=a1.at[z], send_sem=z_send.at[d], recv_sem=z_recv.at[z],
            device_id={"ma": z_peers[d][0], "freq": y}, device_id_type=MESH,
        )

    for d in (4, 3, 5, 2, 6, 1, 7):
        z_copy(d).start()

    g_ref[y] = share.astype(BF16)

    def ag_copy(d):
        return pltpu.make_async_remote_copy(
            src_ref=g_ref.at[y], dst_ref=g_ref.at[y], send_sem=ag_send.at[d], recv_sem=ag_recv.at[y],
            device_id={"ma": ma, "freq": ys[d]}, device_id_type=MESH,
        )

    for d in (2, 1, 3):
        ag_copy(d).start()

    for d in range(1, NZ):
        src = z_peers[d][1]
        pltpu.make_async_remote_copy(
            src_ref=a1.at[z], dst_ref=a1.at[src], send_sem=z_send.at[d], recv_sem=z_recv.at[src],
            device_id={"ma": z_peers[d][0], "freq": y}, device_id_type=MESH,
        ).wait_recv()
    total = a1[0]
    for i in range(1, NZ):
        total = total + a1[i]

    q = (x * NY + y) * NCORE + core
    a2[q] = total

    def w_copy(i):
        return pltpu.make_async_remote_copy(
            src_ref=a2.at[q], dst_ref=a2.at[q], send_sem=w_send.at[i], recv_sem=w_recv.at[q],
            device_id={"ma": w_peers[i][0], "freq": w_peers[i][1]}, device_id_type=MESH,
        )

    for i in range(len(w_peers)):
        w_copy(i).start()
    for d in range(1, NX * NY * NCORE):
        src = lax.rem(q + d, NX * NY * NCORE)
        pltpu.make_async_remote_copy(
            src_ref=a2.at[q], dst_ref=a2.at[src], send_sem=w_send.at[d - 1], recv_sem=w_recv.at[src],
            device_id={"ma": ma, "freq": ys[1]}, device_id_type=MESH,
        ).wait_recv()
    total = a2[0]
    for i in range(1, NX * NY * NCORE):
        total = total + a2[i]
    s_ref[...] = 1.0 / jnp.sqrt(total[:parts] / jnp.maximum(total[parts:], 1.0) + 1e-06)

    for d in range(1, NY):
        src = ys[d]
        pltpu.make_async_remote_copy(
            src_ref=g_ref.at[y], dst_ref=g_ref.at[src], send_sem=ag_send.at[d], recv_sem=ag_recv.at[src],
            device_id={"ma": ma, "freq": src}, device_id_type=MESH,
        ).wait_recv()
    for m in range(modes):
        for h in range(2):
            @pl.when(2 * m + h != y)
            def _():
                rs_copy(m, h).wait_send()
    for d in range(1, NY):
        ag_copy(d).wait_send()
    for d in range(1, NZ):
        z_copy(d).wait_send()
    for i in range(len(w_peers)):
        w_copy(i).wait_send()


def filter_kernel(ret_ref, g_ref, s_ref, eb, c_ref, o_hbm, cf, ob, o_sem):
    modes, freqs = eb.shape[:2]
    blocks = ob.shape[1] // freqs
    kmax = c_ref.shape[3]
    rows = cf.shape[1]
    half = rows // 2
    parts = kmax // LANES

    def o_copy(m, f, b):
        j = f * blocks + b
        return pltpu.make_async_copy(
            ob.at[m, j], o_hbm.at[m, :, f, :, pl.ds(b * LANES, LANES)], o_sem.at[m, j]
        )

    scale = jnp.concatenate([s_ref[pl.ds(p, 1), :] for p in range(parts)], axis=1)
    for m in range(modes):
        keep = (lax.broadcasted_iota(jnp.int32, (1, kmax), 1) < ret_ref[m]).astype(F32)
        gain = keep * scale
        c = jnp.concatenate([g_ref[2 * m], g_ref[2 * m + 1]], axis=0).astype(F32) * gain
        for p in range(parts):
            cf[p] = c[:, p * LANES : (p + 1) * LANES]
        lhs_re = c.astype(BF16)
        lhs_im = pair_turn(c, 1.0).astype(BF16)
        for part in range(2):
            c_ref[m, part] = jnp.concatenate(
                [cf[p, pl.ds(part, half, stride=2), :] for p in range(parts)], axis=1
            ).astype(BF16)
        for f in range(freqs):
            dims = (((1,), (1,)), ((), ()))
            out = lax.dot_general(lhs_re, eb[m, f, 0], dims, preferred_element_type=F32)
            out = out + lax.dot_general(lhs_im, eb[m, f, 1], dims, preferred_element_type=F32)
            for b in range(blocks):
                ob.at[m, f * blocks + b].reshape(rows, LANES)[...] = out[:, b * LANES : (b + 1) * LANES].astype(BF16)
                o_copy(m, f, b).start()
    for m in range(modes):
        for f in range(freqs):
            for b in range(blocks):
                o_copy(m, f, b).wait()


def per_device(visibilities, eigenmodes, retained):
    modes, samples, freqs, _, base = visibilities.shape
    kmax = eigenmodes.shape[-1]
    blocks = base // LANES
    rows = 2 * samples
    half = rows // 2
    group = NX * NY * NCORE
    visibilities, eigenmodes, retained = (
        pltpu.with_memory_space_constraint(a, pltpu.HBM) for a in (visibilities, eigenmodes, retained)
    )
    any_spec = pl.BlockSpec(memory_space=pl.ANY)
    vmem_spec = pl.BlockSpec(memory_space=pltpu.VMEM)
    smem_spec = pl.BlockSpec(memory_space=pltpu.SMEM)
    dma = pltpu.SemaphoreType.DMA
    flops = 2 * modes * rows * freqs * 2 * base * kmax
    gathered, scale, vectors = pl.pallas_call(
        project_kernel,
        out_shape=(
            jax.ShapeDtypeStruct((NY, half, kmax), BF16),
            jax.ShapeDtypeStruct((kmax // LANES, LANES), F32),
            jax.ShapeDtypeStruct((modes, freqs, 2, base, kmax), BF16),
        ),
        in_specs=[smem_spec, any_spec, any_spec],
        out_specs=(vmem_spec, vmem_spec, vmem_spec),
        scratch_shapes=[
            pltpu.VMEM((modes, freqs * blocks, samples, 2, LANES), BF16),
            pltpu.VMEM((rows, kmax), F32),
            pltpu.VMEM((rows, kmax), F32),
            pltpu.VMEM((modes, rows, kmax), F32),
            pltpu.VMEM((modes, rows, kmax), BF16),
            pltpu.VMEM((NY, half, kmax), BF16),
            pltpu.VMEM((NZ, 2 * kmax // LANES, LANES), F32),
            pltpu.VMEM((group, 2 * kmax // LANES, LANES), F32),
            dma((modes, freqs * blocks)),
            dma((modes, freqs)),
            dma((NY,)), dma((NY,)),
            dma((NY,)), dma((NY,)),
            dma((NZ,)), dma((NZ,)),
            dma((group,)), dma((group,)),
        ],
        compiler_params=pltpu.CompilerParams(
            collective_id=0, has_side_effects=True, vmem_limit_bytes=24 << 20
        ),
        cost_estimate=pl.CostEstimate(flops=flops, bytes_accessed=8 << 20, transcendentals=0),
    )(retained, visibilities, eigenmodes)
    coefficients, filtered = pl.pallas_call(
        filter_kernel,
        out_shape=(
            jax.ShapeDtypeStruct((modes, 2, samples, kmax), BF16),
            jax.ShapeDtypeStruct((modes, samples, freqs, 2, base), BF16),
        ),
        in_specs=[smem_spec, vmem_spec, vmem_spec, vmem_spec],
        out_specs=(vmem_spec, any_spec),
        scratch_shapes=[
            pltpu.VMEM((kmax // LANES, rows, LANES), F32),
            pltpu.VMEM((modes, freqs * blocks, samples, 2, LANES), BF16),
            dma((modes, freqs * blocks)),
        ],
        compiler_params=pltpu.CompilerParams(vmem_limit_bytes=24 << 20),
        cost_estimate=pl.CostEstimate(flops=flops, bytes_accessed=8 << 20, transcendentals=0),
    )(retained, gathered, scale, vectors)
    return coefficients, filtered


def solution(mesh):
    return jax.shard_map(
        per_device,
        mesh=mesh,
        in_specs=(P("ma", None, "freq", None, None), P("ma", "freq", None, None, None), P("ma")),
        out_specs=(P("ma", None, None, None), P("ma", None, "freq", None, None)),
        check_vma=False,
    )
```

```python
import functools

import jax
import jax.numpy as jnp
from jax import lax
from jax.experimental import pallas as pl
from jax.experimental.pallas import tpu as pltpu
from jax.sharding import PartitionSpec as P

MESH = pl.DeviceIdType.MESH
BF16, F32 = jnp.bfloat16, jnp.float32
NX, NZ, NCORE, NY = 4, 8, 2, 4
LANES = 128


def pair_turn(x, odd_sign):
    rows, cols = x.shape
    tiles = x.reshape(rows // 8, 8, cols)
    even = lax.broadcasted_iota(jnp.int32, tiles.shape, 1) % 2 == 0
    turned = jnp.where(even, -odd_sign * pltpu.roll(tiles, 7, 1), odd_sign * pltpu.roll(tiles, 1, 1))
    return turned.reshape(rows, cols)


def project_kernel(
    ret_ref, x_hbm, e_hbm, g_ref, s_ref, eb,
    xt, xb, acc_re, acc_im, pf, sbuf, rbuf, a1, a2,
    x_sem, t_sem, e_sem, rs_send, rs_recv, ag_send, ag_recv, z_send, z_recv, w_send, w_recv,
):
    modes, freqs, half = xb.shape[0], e_hbm.shape[1], rbuf.shape[1]
    blocks = xb.shape[1] // freqs
    rows, kmax = sbuf.shape[1:]
    ma = lax.axis_index("ma")
    y = lax.axis_index("freq")
    core = lax.rem(ma, NCORE)
    z = lax.rem(ma // NCORE, NZ)
    x = ma // (NCORE * NZ)

    def x_copy(m, f, b):
        j = f * blocks + b
        return pltpu.make_async_copy(
            x_hbm.at[m, :, f, :, pl.ds(b * LANES, LANES)], xt.at[m, j], x_sem.at[m, j]
        )

    def t_copy(m, f, b):
        j = f * blocks + b
        return pltpu.make_async_copy(xt.at[m, j].reshape(rows, LANES), xb.at[m, j], t_sem.at[m, j])

    def take(u):
        m, f = divmod(u, freqs)
        for b in range(blocks):
            x_copy(m, f, b).wait()
            t_copy(m, f, b).start()

    def e_copy(m, f):
        return pltpu.make_async_copy(e_hbm.at[m, f], eb.at[m, f], e_sem.at[m, f])

    for m in range(modes):
        for f in range(freqs):
            e_copy(m, f).start()
            for b in range(blocks):
                x_copy(m, f, b).start()

    z_peers = [((x * NZ + lax.rem(z + d, NZ)) * NCORE + core, lax.rem(z + d, NZ)) for d in range(NZ)]
    xs = [lax.rem(x + d, NX) for d in range(NX)]
    ys = [lax.rem(y + d, NY) for d in range(NY)]
    cs = [core, 1 - core]
    far = [2, 1, 3, 0]
    w_peers = [
        ((xs[dx] * NZ + z) * NCORE + cs[dc], ys[dy])
        for dx in far for dy in far for dc in (1, 0)
        if (dx, dy, dc) != (0, 0, 0)
    ]
    barrier = pltpu.get_barrier_semaphore()
    for peer in w_peers:
        pl.semaphore_signal(barrier, inc=1, device_id={"ma": peer[0], "freq": peer[1]}, device_id_type=MESH)
    for d in range(1, NZ):
        pl.semaphore_signal(barrier, inc=1, device_id={"ma": z_peers[d][0], "freq": y}, device_id_type=MESH)

    def rs_copy(m, h):
        t = 2 * m + h
        return pltpu.make_async_remote_copy(
            src_ref=sbuf.at[m, pl.ds(h * half, half)], dst_ref=rbuf.at[y],
            send_sem=rs_send.at[t], recv_sem=rs_recv.at[y],
            device_id={"ma": ma, "freq": t}, device_id_type=MESH,
        )

    for m in range(modes):
        for f in range(freqs):
            u = m * freqs + f
            if u == 0:
                take(0)
            if u + 1 < modes * freqs:
                take(u + 1)
            e_copy(m, f).wait()
            for b in range(blocks):
                t_copy(m, f, b).wait()
            lhs = jnp.concatenate([xb[m, f * blocks + b] for b in range(blocks)], axis=1)
            d_re = jnp.dot(lhs, eb[m, f, 0], preferred_element_type=F32)
            d_im = jnp.dot(lhs, eb[m, f, 1], preferred_element_type=F32)
            if f == 0:
                acc_re[...] = d_re
                acc_im[...] = d_im
            else:
                acc_re[...] += d_re
                acc_im[...] += d_im
        proj = acc_re[...] + pair_turn(acc_im[...], -1.0)
        pf[m] = proj
        sbuf[m] = proj.astype(BF16)
        if m == 0:
            pl.semaphore_wait(barrier, len(w_peers) + NZ - 1)
        for h in range(2):
            @pl.when(2 * m + h != y)
            def _():
                rs_copy(m, h).start()

    share = pf[y // 2, pl.ds(lax.rem(y, 2) * half, half), :]
    for d in range(1, NY):
        src = ys[d]
        pltpu.make_async_remote_copy(
            src_ref=sbuf.at[0, pl.ds(0, half)], dst_ref=rbuf.at[src],
            send_sem=rs_send.at[src], recv_sem=rs_recv.at[src],
            device_id={"ma": ma, "freq": src}, device_id_type=MESH,
        ).wait_recv()
        share = share + rbuf[src].astype(F32)
    cut = ret_ref[y // 2]
    keep = (lax.broadcasted_iota(jnp.int32, (1, kmax), 1) < cut).astype(F32)
    power = keep * jnp.sum(share * share, axis=0, keepdims=True)
    count = keep * (half // 2)
    parts = kmax // LANES
    for p in range(parts):
        a1[z, pl.ds(p, 1), :] = power[:, p * LANES : (p + 1) * LANES]
        a1[z, pl.ds(parts + p, 1), :] = count[:, p * LANES : (p + 1) * LANES]

    def z_copy(d):
        return pltpu.make_async_remote_copy(
            src_ref=a1.at[z], dst_ref=a1.at[z], send_sem=z_send.at[d], recv_sem=z_recv.at[z],
            device_id={"ma": z_peers[d][0], "freq": y}, device_id_type=MESH,
        )

    for d in (4, 3, 5, 2, 6, 1, 7):
        z_copy(d).start()

    g_ref[y] = share.astype(BF16)

    def ag_copy(d):
        return pltpu.make_async_remote_copy(
            src_ref=g_ref.at[y], dst_ref=g_ref.at[y], send_sem=ag_send.at[d], recv_sem=ag_recv.at[y],
            device_id={"ma": ma, "freq": ys[d]}, device_id_type=MESH,
        )

    for d in (2, 1, 3):
        ag_copy(d).start()

    for d in range(1, NZ):
        src = z_peers[d][1]
        pltpu.make_async_remote_copy(
            src_ref=a1.at[z], dst_ref=a1.at[src], send_sem=z_send.at[d], recv_sem=z_recv.at[src],
            device_id={"ma": z_peers[d][0], "freq": y}, device_id_type=MESH,
        ).wait_recv()
    total = a1[0]
    for i in range(1, NZ):
        total = total + a1[i]

    q = (x * NY + y) * NCORE + core
    a2[q] = total

    def w_copy(i):
        return pltpu.make_async_remote_copy(
            src_ref=a2.at[q], dst_ref=a2.at[q], send_sem=w_send.at[i], recv_sem=w_recv.at[q],
            device_id={"ma": w_peers[i][0], "freq": w_peers[i][1]}, device_id_type=MESH,
        )

    for i in range(len(w_peers)):
        w_copy(i).start()
    for d in range(1, NX * NY * NCORE):
        src = lax.rem(q + d, NX * NY * NCORE)
        pltpu.make_async_remote_copy(
            src_ref=a2.at[q], dst_ref=a2.at[src], send_sem=w_send.at[d - 1], recv_sem=w_recv.at[src],
            device_id={"ma": ma, "freq": ys[1]}, device_id_type=MESH,
        ).wait_recv()
    total = a2[0]
    for i in range(1, NX * NY * NCORE):
        total = total + a2[i]
    s_ref[...] = 1.0 / jnp.sqrt(total[:parts] / jnp.maximum(total[parts:], 1.0) + 1e-06)

    for d in range(1, NY):
        src = ys[d]
        pltpu.make_async_remote_copy(
            src_ref=g_ref.at[y], dst_ref=g_ref.at[src], send_sem=ag_send.at[d], recv_sem=ag_recv.at[src],
            device_id={"ma": ma, "freq": src}, device_id_type=MESH,
        ).wait_recv()
    for m in range(modes):
        for h in range(2):
            @pl.when(2 * m + h != y)
            def _():
                rs_copy(m, h).wait_send()
    for d in range(1, NY):
        ag_copy(d).wait_send()
    for d in range(1, NZ):
        z_copy(d).wait_send()
    for i in range(len(w_peers)):
        w_copy(i).wait_send()


def filter_kernel(ret_ref, g_ref, s_ref, eb, c_ref, o_hbm, cf, ob, ot, t_sem, o_sem):
    modes, freqs = eb.shape[:2]
    blocks = ob.shape[1] // freqs
    kmax = c_ref.shape[3]
    rows = cf.shape[1]
    half = rows // 2
    parts = kmax // LANES

    def o_copy(m, f, b):
        j = f * blocks + b
        return pltpu.make_async_copy(
            ot.at[m, j], o_hbm.at[m, :, f, :, pl.ds(b * LANES, LANES)], o_sem.at[m, j]
        )

    def t_copy(m, f, b):
        j = f * blocks + b
        return pltpu.make_async_copy(ob.at[m, j], ot.at[m, j].reshape(rows, LANES), t_sem.at[m, j])

    def give(u):
        m, f = divmod(u, freqs)
        for b in range(blocks):
            t_copy(m, f, b).wait()
            o_copy(m, f, b).start()

    scale = jnp.concatenate([s_ref[pl.ds(p, 1), :] for p in range(parts)], axis=1)
    for m in range(modes):
        keep = (lax.broadcasted_iota(jnp.int32, (1, kmax), 1) < ret_ref[m]).astype(F32)
        gain = keep * scale
        c = jnp.concatenate([g_ref[2 * m], g_ref[2 * m + 1]], axis=0).astype(F32) * gain
        for p in range(parts):
            cf[p] = c[:, p * LANES : (p + 1) * LANES]
        lhs_re = c.astype(BF16)
        lhs_im = pair_turn(c, 1.0).astype(BF16)
        for part in range(2):
            c_ref[m, part] = jnp.concatenate(
                [cf[p, pl.ds(part, half, stride=2), :] for p in range(parts)], axis=1
            ).astype(BF16)
        for f in range(freqs):
            dims = (((1,), (1,)), ((), ()))
            out = lax.dot_general(lhs_re, eb[m, f, 0], dims, preferred_element_type=F32)
            out = out + lax.dot_general(lhs_im, eb[m, f, 1], dims, preferred_element_type=F32)
            for b in range(blocks):
                ob[m, f * blocks + b] = out[:, b * LANES : (b + 1) * LANES].astype(BF16)
                t_copy(m, f, b).start()
            if m + f > 0:
                give(m * freqs + f - 1)
    give(modes * freqs - 1)
    for m in range(modes):
        for f in range(freqs):
            for b in range(blocks):
                o_copy(m, f, b).wait()


def per_device(visibilities, eigenmodes, retained):
    modes, samples, freqs, _, base = visibilities.shape
    kmax = eigenmodes.shape[-1]
    blocks = base // LANES
    rows = 2 * samples
    half = rows // 2
    group = NX * NY * NCORE
    visibilities, eigenmodes, retained = (
        pltpu.with_memory_space_constraint(a, pltpu.HBM) for a in (visibilities, eigenmodes, retained)
    )
    any_spec = pl.BlockSpec(memory_space=pl.ANY)
    vmem_spec = pl.BlockSpec(memory_space=pltpu.VMEM)
    smem_spec = pl.BlockSpec(memory_space=pltpu.SMEM)
    dma = pltpu.SemaphoreType.DMA
    flops = 2 * modes * rows * freqs * 2 * base * kmax
    gathered, scale, vectors = pl.pallas_call(
        project_kernel,
        out_shape=(
            jax.ShapeDtypeStruct((NY, half, kmax), BF16),
            jax.ShapeDtypeStruct((kmax // LANES, LANES), F32),
            jax.ShapeDtypeStruct((modes, freqs, 2, base, kmax), BF16),
        ),
        in_specs=[smem_spec, any_spec, any_spec],
        out_specs=(vmem_spec, vmem_spec, vmem_spec),
        scratch_shapes=[
            pltpu.VMEM((modes, freqs * blocks, samples, 2, LANES), BF16),
            pltpu.VMEM((modes, freqs * blocks, rows, LANES), BF16),
            pltpu.VMEM((rows, kmax), F32),
            pltpu.VMEM((rows, kmax), F32),
            pltpu.VMEM((modes, rows, kmax), F32),
            pltpu.VMEM((modes, rows, kmax), BF16),
            pltpu.VMEM((NY, half, kmax), BF16),
            pltpu.VMEM((NZ, 2 * kmax // LANES, LANES), F32),
            pltpu.VMEM((group, 2 * kmax // LANES, LANES), F32),
            dma((modes, freqs * blocks)),
            dma((modes, freqs * blocks)),
            dma((modes, freqs)),
            dma((NY,)), dma((NY,)),
            dma((NY,)), dma((NY,)),
            dma((NZ,)), dma((NZ,)),
            dma((group,)), dma((group,)),
        ],
        compiler_params=pltpu.CompilerParams(
            collective_id=0, has_side_effects=True, vmem_limit_bytes=24 << 20
        ),
        cost_estimate=pl.CostEstimate(flops=flops, bytes_accessed=8 << 20, transcendentals=0),
    )(retained, visibilities, eigenmodes)
    coefficients, filtered = pl.pallas_call(
        filter_kernel,
        out_shape=(
            jax.ShapeDtypeStruct((modes, 2, samples, kmax), BF16),
            jax.ShapeDtypeStruct((modes, samples, freqs, 2, base), BF16),
        ),
        in_specs=[smem_spec, vmem_spec, vmem_spec, vmem_spec],
        out_specs=(vmem_spec, any_spec),
        scratch_shapes=[
            pltpu.VMEM((kmax // LANES, rows, LANES), F32),
            pltpu.VMEM((modes, freqs * blocks, rows, LANES), BF16),
            pltpu.VMEM((modes, freqs * blocks, samples, 2, LANES), BF16),
            dma((modes, freqs * blocks)),
            dma((modes, freqs * blocks)),
        ],
        compiler_params=pltpu.CompilerParams(vmem_limit_bytes=24 << 20),
        cost_estimate=pl.CostEstimate(flops=flops, bytes_accessed=8 << 20, transcendentals=0),
    )(retained, gathered, scale, vectors)
    return coefficients, filtered


def solution(mesh):
    return jax.shard_map(
        per_device,
        mesh=mesh,
        in_specs=(P("ma", None, "freq", None, None), P("ma", "freq", None, None, None), P("ma")),
        out_specs=(P("ma", None, None, None), P("ma", None, "freq", None, None)),
        check_vma=False,
    )
```

```python
import functools

import jax
import jax.numpy as jnp
from jax import lax
from jax.experimental import pallas as pl
from jax.experimental.pallas import tpu as pltpu
from jax.sharding import PartitionSpec as P

MESH = pl.DeviceIdType.MESH
BF16, F32 = jnp.bfloat16, jnp.float32
NX, NZ, NCORE, NY = 4, 8, 2, 4
LANES = 128


def project_kernel(
    ret_hbm, x_hbm, e_hbm, g_ref, s_ref, eb,
    ret_ref, xb, acc_re, acc_im, pf, sbuf, rbuf, a1, a2,
    ret_sem, x_sem, e_sem, rs_send, rs_recv, ag_send, ag_recv, z_send, z_recv, w_send, w_recv,
):
    modes, freqs, _, base, kmax = eb.shape
    samples = pf.shape[2]
    half = samples // 2
    parts = kmax // LANES
    ma = lax.axis_index("ma")
    y = lax.axis_index("freq")
    core = lax.rem(ma, NCORE)
    z = lax.rem(ma // NCORE, NZ)
    x = ma // (NCORE * NZ)

    def x_copy(m, f):
        return pltpu.make_async_copy(x_hbm.at[m, :, f], xb.at[m, f], x_sem.at[m, f])

    def e_copy(m, f):
        return pltpu.make_async_copy(e_hbm.at[m, f], eb.at[m, f], e_sem.at[m, f])

    order = (1 - y // 2, y // 2)
    for m in order:
        for f in range(freqs):
            x_copy(m, f).start()
            e_copy(m, f).start()
    ret_copy = pltpu.make_async_copy(ret_hbm, ret_ref, ret_sem)
    ret_copy.start()

    z_peers = [((x * NZ + lax.rem(z + d, NZ)) * NCORE + core, lax.rem(z + d, NZ)) for d in range(NZ)]
    xs = [lax.rem(x + d, NX) for d in range(NX)]
    ys = [lax.rem(y + d, NY) for d in range(NY)]
    cs = [core, 1 - core]
    far = [2, 1, 3, 0]
    w_peers = [
        ((xs[dx] * NZ + z) * NCORE + cs[dc], ys[dy])
        for dx in far for dy in far for dc in (1, 0)
        if (dx, dy, dc) != (0, 0, 0)
    ]
    barrier = pltpu.get_barrier_semaphore()
    for peer in w_peers:
        pl.semaphore_signal(barrier, inc=1, device_id={"ma": peer[0], "freq": peer[1]}, device_id_type=MESH)
    for d in range(1, NZ):
        pl.semaphore_signal(barrier, inc=1, device_id={"ma": z_peers[d][0], "freq": y}, device_id_type=MESH)

    def rs_copy(i, t):
        return pltpu.make_async_remote_copy(
            src_ref=sbuf.at[i], dst_ref=rbuf.at[y], send_sem=rs_send.at[i], recv_sem=rs_recv.at[y],
            device_id={"ma": ma, "freq": t}, device_id_type=MESH,
        )

    mine = lax.rem(y, 2)
    rs_copies = (rs_copy(0, 2 * order[0] + mine), rs_copy(1, 2 * order[0] + 1 - mine), rs_copy(2, 2 * order[1] + 1 - mine))

    def hand_over(i, slot, h):
        for c in range(2):
            sbuf[i, c] = pf[slot, c, pl.ds(pl.multiple_of(h * half, 32), half), :].astype(BF16)
        rs_copies[i].start()

    for slot in range(modes):
        m = order[slot]
        for f in range(freqs):
            x_copy(m, f).wait()
            e_copy(m, f).wait()
            lhs = xb[m, f].reshape(2 * samples, base)
            for c, acc in ((0, acc_re), (1, acc_im)):
                d = jnp.dot(lhs, eb[m, f, c], preferred_element_type=F32)
                for p in range(parts):
                    piece = d[:, p * LANES : (p + 1) * LANES]
                    acc[slot, p] = piece if f == 0 else acc[slot, p] + piece
        even, odd = pl.ds(0, samples, stride=2), pl.ds(1, samples, stride=2)
        for p in range(parts):
            lanes = slice(p * LANES, (p + 1) * LANES)
            pf[slot, 0, :, lanes] = acc_re[slot, p, even, :] + acc_im[slot, p, odd, :]
            pf[slot, 1, :, lanes] = acc_re[slot, p, odd, :] - acc_im[slot, p, even, :]
        if slot == 0:
            pl.semaphore_wait(barrier, len(w_peers) + NZ - 1)
            hand_over(0, 0, mine)
            hand_over(1, 0, 1 - mine)
        else:
            hand_over(2, 1, 1 - mine)

    share = pf[1, :, pl.ds(pl.multiple_of(mine * half, 32), half), :]
    for d in range(1, NY):
        src = ys[d]
        pltpu.make_async_remote_copy(
            src_ref=sbuf.at[0], dst_ref=rbuf.at[src],
            send_sem=rs_send.at[d - 1], recv_sem=rs_recv.at[src],
            device_id={"ma": ma, "freq": src}, device_id_type=MESH,
        ).wait_recv()
        share = share + rbuf[src].astype(F32)
    ret_copy.wait()
    ranks = lax.broadcasted_iota(jnp.int32, (1, kmax), 1)
    keep = (ranks < ret_ref[y // 2]).astype(F32)
    power = keep * jnp.sum(share[0] * share[0] + share[1] * share[1], axis=0, keepdims=True)
    count = keep * half
    for p in range(parts):
        a1[z, pl.ds(p, 1), :] = power[:, p * LANES : (p + 1) * LANES]
        a1[z, pl.ds(parts + p, 1), :] = count[:, p * LANES : (p + 1) * LANES]

    def z_copy(d):
        return pltpu.make_async_remote_copy(
            src_ref=a1.at[z], dst_ref=a1.at[z], send_sem=z_send.at[d], recv_sem=z_recv.at[z],
            device_id={"ma": z_peers[d][0], "freq": y}, device_id_type=MESH,
        )

    for d in (4, 3, 5, 2, 6, 1, 7):
        z_copy(d).start()

    g_ref[y] = share.astype(BF16)

    def ag_copy(d):
        return pltpu.make_async_remote_copy(
            src_ref=g_ref.at[y], dst_ref=g_ref.at[y], send_sem=ag_send.at[d], recv_sem=ag_recv.at[y],
            device_id={"ma": ma, "freq": ys[d]}, device_id_type=MESH,
        )

    for d in (2, 1, 3):
        ag_copy(d).start()

    for d in range(1, NZ):
        src = z_peers[d][1]
        pltpu.make_async_remote_copy(
            src_ref=a1.at[z], dst_ref=a1.at[src], send_sem=z_send.at[d], recv_sem=z_recv.at[src],
            device_id={"ma": z_peers[d][0], "freq": y}, device_id_type=MESH,
        ).wait_recv()
    total = a1[0]
    for i in range(1, NZ):
        total = total + a1[i]

    q = (x * NY + y) * NCORE + core
    a2[q] = total

    def w_copy(i):
        return pltpu.make_async_remote_copy(
            src_ref=a2.at[q], dst_ref=a2.at[q], send_sem=w_send.at[i], recv_sem=w_recv.at[q],
            device_id={"ma": w_peers[i][0], "freq": w_peers[i][1]}, device_id_type=MESH,
        )

    for i in range(len(w_peers)):
        w_copy(i).start()
    for d in range(1, NX * NY * NCORE):
        src = lax.rem(q + d, NX * NY * NCORE)
        pltpu.make_async_remote_copy(
            src_ref=a2.at[q], dst_ref=a2.at[src], send_sem=w_send.at[d - 1], recv_sem=w_recv.at[src],
            device_id={"ma": ma, "freq": ys[1]}, device_id_type=MESH,
        ).wait_recv()
    total = a2[0]
    for i in range(1, NX * NY * NCORE):
        total = total + a2[i]
    scale = 1.0 / jnp.sqrt(total[:parts] / jnp.maximum(total[parts:], 1.0) + 1e-06)
    scale = jnp.concatenate([scale[p : p + 1, :] for p in range(parts)], axis=1)
    for m in range(modes):
        s_ref[pl.ds(m, 1), :] = (ranks < ret_ref[m]).astype(F32) * scale

    for d in range(1, NY):
        src = ys[d]
        pltpu.make_async_remote_copy(
            src_ref=g_ref.at[y], dst_ref=g_ref.at[src], send_sem=ag_send.at[d], recv_sem=ag_recv.at[src],
            device_id={"ma": ma, "freq": src}, device_id_type=MESH,
        ).wait_recv()
    for copy in rs_copies:
        copy.wait_send()
    for d in range(1, NY):
        ag_copy(d).wait_send()
    for d in range(1, NZ):
        z_copy(d).wait_send()
    for i in range(len(w_peers)):
        w_copy(i).wait_send()


def filter_kernel(g_ref, s_ref, eb, c_hbm, o_hbm, cb, of, ob, c_sem, o_sem):
    modes, freqs, _, base, kmax = eb.shape
    samples = cb.shape[2]
    blocks = base // LANES
    stride = 2 * freqs
    wide = 2 * LANES

    def o_copy(m, b):
        slab = o_hbm.at[m].reshape(samples * stride, base).at[:, pl.ds(b * LANES, LANES)]
        return pltpu.make_async_copy(ob.at[m, b], slab, o_sem.at[m, b])

    def c_copy(m):
        return pltpu.make_async_copy(cb.at[m], c_hbm.at[m], c_sem.at[m])

    for m in range(modes):
        gain = s_ref[pl.ds(m, 1), :]
        re, im = (
            (jnp.concatenate([g_ref[2 * m, c], g_ref[2 * m + 1, c]], axis=0).astype(F32) * gain).astype(BF16)
            for c in range(2)
        )
        cb[m, 0] = re
        cb[m, 1] = im
        c_copy(m).start()
        lhs = jnp.concatenate(
            [jnp.concatenate([re, -im], axis=1), jnp.concatenate([im, re], axis=1)], axis=0
        )
        for p in range(blocks // 2):
            for f in range(freqs):
                rhs = jnp.concatenate([eb[m, f, c, p * wide : (p + 1) * wide, :] for c in range(2)], axis=1)
                out = lax.dot_general(lhs, rhs, (((1,), (1,)), ((), ())), preferred_element_type=F32)
                for c in range(2):
                    for i in range(2):
                        of[m, 2 * p + i, pl.ds(2 * f + c, samples, stride=stride), :] = out[
                            c * samples : (c + 1) * samples, i * LANES : (i + 1) * LANES
                        ]
            for b in (2 * p, 2 * p + 1):
                ob[m, b] = of[m, b].astype(BF16)
                o_copy(m, b).start()
    for m in range(modes):
        c_copy(m).wait()
        for b in range(blocks):
            o_copy(m, b).wait()


def per_device(visibilities, eigenmodes, retained):
    modes, samples, freqs, _, base = visibilities.shape
    kmax = eigenmodes.shape[-1]
    blocks = base // LANES
    rows = 2 * samples
    half = samples // 2
    slab = samples * freqs * 2
    group = NX * NY * NCORE
    visibilities, eigenmodes, retained = (
        pltpu.with_memory_space_constraint(a, pltpu.HBM) for a in (visibilities, eigenmodes, retained)
    )
    any_spec = pl.BlockSpec(memory_space=pl.ANY)
    vmem_spec = pl.BlockSpec(memory_space=pltpu.VMEM)
    dma = pltpu.SemaphoreType.DMA
    flops = 2 * modes * rows * freqs * 2 * base * kmax
    gathered, scale, vectors = pl.pallas_call(
        project_kernel,
        out_shape=(
            jax.ShapeDtypeStruct((NY, 2, half, kmax), BF16),
            jax.ShapeDtypeStruct((modes, kmax), F32),
            jax.ShapeDtypeStruct((modes, freqs, 2, base, kmax), BF16),
        ),
        in_specs=[any_spec, any_spec, any_spec],
        out_specs=(vmem_spec, vmem_spec, vmem_spec),
        scratch_shapes=[
            pltpu.SMEM((modes,), jnp.int32),
            pltpu.VMEM((modes, freqs, samples, 2, base), BF16),
            pltpu.VMEM((modes, kmax // LANES, rows, LANES), F32),
            pltpu.VMEM((modes, kmax // LANES, rows, LANES), F32),
            pltpu.VMEM((modes, 2, samples, kmax), F32),
            pltpu.VMEM((NY - 1, 2, half, kmax), BF16),
            pltpu.VMEM((NY, 2, half, kmax), BF16),
            pltpu.VMEM((NZ, 2 * kmax // LANES, LANES), F32),
            pltpu.VMEM((group, 2 * kmax // LANES, LANES), F32),
            dma,
            dma((modes, freqs)),
            dma((modes, freqs)),
            dma((NY - 1,)), dma((NY,)),
            dma((NY,)), dma((NY,)),
            dma((NZ,)), dma((NZ,)),
            dma((group,)), dma((group,)),
        ],
        compiler_params=pltpu.CompilerParams(
            collective_id=0, has_side_effects=True, vmem_limit_bytes=32 << 20
        ),
        cost_estimate=pl.CostEstimate(flops=flops, bytes_accessed=8 << 20, transcendentals=0),
    )(retained, visibilities, eigenmodes)
    coefficients, filtered = pl.pallas_call(
        filter_kernel,
        out_shape=(
            jax.ShapeDtypeStruct((modes, 2, samples, kmax), BF16),
            jax.ShapeDtypeStruct((modes, samples, freqs, 2, base), BF16),
        ),
        in_specs=[vmem_spec, vmem_spec, vmem_spec],
        out_specs=(any_spec, any_spec),
        scratch_shapes=[
            pltpu.VMEM((modes, 2, samples, kmax), BF16),
            pltpu.VMEM((modes, blocks, slab, LANES), F32),
            pltpu.VMEM((modes, blocks, slab, LANES), BF16),
            dma((modes,)),
            dma((modes, blocks)),
        ],
        compiler_params=pltpu.CompilerParams(vmem_limit_bytes=32 << 20),
        cost_estimate=pl.CostEstimate(flops=flops, bytes_accessed=8 << 20, transcendentals=0),
    )(gathered, scale, vectors)
    return coefficients, filtered


def solution(mesh):
    return jax.shard_map(
        per_device,
        mesh=mesh,
        in_specs=(P("ma", None, "freq", None, None), P("ma", "freq", None, None, None), P("ma")),
        out_specs=(P("ma", None, None, None), P("ma", None, "freq", None, None)),
        check_vma=False,
    )
```

```python
import functools

import jax
import jax.numpy as jnp
from jax import lax
from jax.experimental import pallas as pl
from jax.experimental.pallas import tpu as pltpu
from jax.sharding import PartitionSpec as P

MESH = pl.DeviceIdType.MESH
BF16, F32 = jnp.bfloat16, jnp.float32
NX, NZ, NCORE, NY = 4, 8, 2, 4
LANES = 128


def project_kernel(
    ret_hbm, x_hbm, e_hbm, g_ref, s_ref, eb,
    ret_ref, xb, xh, acc_re, acc_im, pf, sbuf, rbuf, a1, a2,
    ret_sem, x_sem, xh_sem, e_sem, rs_send, rs_recv, ag_send, ag_recv, z_send, z_recv, w_send, w_recv,
):
    modes, freqs, _, base, kmax = eb.shape
    half = pf.shape[1]
    samples = 2 * half
    parts = kmax // LANES
    ma = lax.axis_index("ma")
    y = lax.axis_index("freq")
    core = lax.rem(ma, NCORE)
    z = lax.rem(ma // NCORE, NZ)
    x = ma // (NCORE * NZ)

    mine = lax.rem(y, 2)
    first, second = 1 - y // 2, y // 2

    def x_copy(f):
        return pltpu.make_async_copy(x_hbm.at[first, :, f], xb.at[f], x_sem.at[f])

    def xh_copy(own, f):
        start = pl.multiple_of((mine if own else 1 - mine) * half, half)
        return pltpu.make_async_copy(x_hbm.at[second, pl.ds(start, half), f], xh.at[own, f], xh_sem.at[own, f])

    def e_copy(m, f):
        return pltpu.make_async_copy(e_hbm.at[m, f], eb.at[m, f], e_sem.at[m, f])

    for f in range(freqs):
        x_copy(f).start()
        e_copy(first, f).start()
    for f in range(freqs):
        xh_copy(0, f).start()
        e_copy(second, f).start()
    for f in range(freqs):
        xh_copy(1, f).start()
    ret_copy = pltpu.make_async_copy(ret_hbm, ret_ref, ret_sem)
    ret_copy.start()

    z_peers = [((x * NZ + lax.rem(z + d, NZ)) * NCORE + core, lax.rem(z + d, NZ)) for d in range(NZ)]
    xs = [lax.rem(x + d, NX) for d in range(NX)]
    ys = [lax.rem(y + d, NY) for d in range(NY)]
    cs = [core, 1 - core]
    far = [2, 1, 3, 0]
    w_peers = [
        ((xs[dx] * NZ + z) * NCORE + cs[dc], ys[dy])
        for dx in far for dy in far for dc in (1, 0)
        if (dx, dy, dc) != (0, 0, 0)
    ]
    barrier = pltpu.get_barrier_semaphore()
    for peer in w_peers:
        pl.semaphore_signal(barrier, inc=1, device_id={"ma": peer[0], "freq": peer[1]}, device_id_type=MESH)
    for d in range(1, NZ):
        pl.semaphore_signal(barrier, inc=1, device_id={"ma": z_peers[d][0], "freq": y}, device_id_type=MESH)

    def rs_copy(i, part, t):
        return pltpu.make_async_remote_copy(
            src_ref=sbuf.at[part], dst_ref=rbuf.at[y], send_sem=rs_send.at[i], recv_sem=rs_recv.at[y],
            device_id={"ma": ma, "freq": t}, device_id_type=MESH,
        )

    rs_copies = (
        rs_copy(0, mine, 2 * first + mine),
        rs_copy(1, 1 - mine, 2 * first + 1 - mine),
        rs_copy(2, 2, 2 * second + 1 - mine),
    )

    def project(unit, m, f, lhs):
        count = lhs.shape[0]
        for c, acc in ((0, acc_re), (1, acc_im)):
            d = jnp.dot(lhs, eb[m, f, c], preferred_element_type=F32)
            for p in range(parts):
                piece = d[:, p * LANES : (p + 1) * LANES]
                acc[unit, p, :count] = piece if f == 0 else acc[unit, p, :count] + piece

    def combine(unit, count, put):
        even, odd = pl.ds(0, count, stride=2), pl.ds(1, count, stride=2)
        for p in range(parts):
            lanes = slice(p * LANES, (p + 1) * LANES)
            put(0, lanes, acc_re[unit, p, even, :] + acc_im[unit, p, odd, :])
            put(1, lanes, acc_re[unit, p, odd, :] - acc_im[unit, p, even, :])

    def put_halves(c, lanes, value):
        for h in range(2):
            sbuf[h, c, :, lanes] = value[h * half : (h + 1) * half].astype(BF16)

    def put_partner(c, lanes, value):
        sbuf[2, c, :, lanes] = value.astype(BF16)

    def put_own(c, lanes, value):
        pf[c, :, lanes] = value

    for f in range(freqs):
        x_copy(f).wait()
        e_copy(first, f).wait()
        project(0, first, f, xb[f].reshape(2 * samples, base))
    combine(0, samples, put_halves)
    pl.semaphore_wait(barrier, len(w_peers) + NZ - 1)
    rs_copies[0].start()
    rs_copies[1].start()
    for f in range(freqs):
        xh_copy(0, f).wait()
        e_copy(second, f).wait()
        project(1, second, f, xh[0, f].reshape(samples, base))
    combine(1, half, put_partner)
    rs_copies[2].start()
    for f in range(freqs):
        xh_copy(1, f).wait()
        project(2, second, f, xh[1, f].reshape(samples, base))
    combine(2, half, put_own)
    share = pf[...]
    for d in range(1, NY):
        src = ys[d]
        pltpu.make_async_remote_copy(
            src_ref=sbuf.at[0], dst_ref=rbuf.at[src],
            send_sem=rs_send.at[d - 1], recv_sem=rs_recv.at[src],
            device_id={"ma": ma, "freq": src}, device_id_type=MESH,
        ).wait_recv()
        share = share + rbuf[src].astype(F32)
    ret_copy.wait()
    ranks = lax.broadcasted_iota(jnp.int32, (1, kmax), 1)
    keep = (ranks < ret_ref[y // 2]).astype(F32)
    power = keep * jnp.sum(share[0] * share[0] + share[1] * share[1], axis=0, keepdims=True)
    count = keep * half
    for p in range(parts):
        a1[z, pl.ds(p, 1), :] = power[:, p * LANES : (p + 1) * LANES]
        a1[z, pl.ds(parts + p, 1), :] = count[:, p * LANES : (p + 1) * LANES]

    def z_copy(d):
        return pltpu.make_async_remote_copy(
            src_ref=a1.at[z], dst_ref=a1.at[z], send_sem=z_send, recv_sem=z_recv,
            device_id={"ma": z_peers[d][0], "freq": y}, device_id_type=MESH,
        )

    for d in (4, 3, 5, 2, 6, 1, 7):
        z_copy(d).start()

    g_ref[y] = share.astype(BF16)

    def ag_copy(d):
        return pltpu.make_async_remote_copy(
            src_ref=g_ref.at[y], dst_ref=g_ref.at[y], send_sem=ag_send.at[d], recv_sem=ag_recv.at[y],
            device_id={"ma": ma, "freq": ys[d]}, device_id_type=MESH,
        )

    for d in (2, 1, 3):
        ag_copy(d).start()

    def settle(ref, count, sem):
        pltpu.make_async_copy(ref.at[pl.ds(0, count)], ref.at[pl.ds(0, count)], sem).wait()

    settle(a1, NZ - 1, z_recv)
    total = a1[0]
    for i in range(1, NZ):
        total = total + a1[i]

    q = (x * NY + y) * NCORE + core
    a2[q] = total

    def w_copy(i):
        return pltpu.make_async_remote_copy(
            src_ref=a2.at[q], dst_ref=a2.at[q], send_sem=w_send, recv_sem=w_recv,
            device_id={"ma": w_peers[i][0], "freq": w_peers[i][1]}, device_id_type=MESH,
        )

    for i in range(len(w_peers)):
        w_copy(i).start()
    settle(a2, len(w_peers), w_recv)
    total = a2[0]
    for i in range(1, NX * NY * NCORE):
        total = total + a2[i]
    scale = 1.0 / jnp.sqrt(total[:parts] / jnp.maximum(total[parts:], 1.0) + 1e-06)
    scale = jnp.concatenate([scale[p : p + 1, :] for p in range(parts)], axis=1)
    for m in range(modes):
        s_ref[pl.ds(m, 1), :] = (ranks < ret_ref[m]).astype(F32) * scale

    for d in range(1, NY):
        src = ys[d]
        pltpu.make_async_remote_copy(
            src_ref=g_ref.at[y], dst_ref=g_ref.at[src], send_sem=ag_send.at[d], recv_sem=ag_recv.at[src],
            device_id={"ma": ma, "freq": src}, device_id_type=MESH,
        ).wait_recv()
    for copy in rs_copies:
        copy.wait_send()
    for d in range(1, NY):
        ag_copy(d).wait_send()
    settle(a1, NZ - 1, z_send)
    settle(a2, len(w_peers), w_send)


def filter_kernel(g_ref, s_ref, eb, c_hbm, o_hbm, cb, of, ob, c_sem, o_sem):
    modes, freqs, _, base, kmax = eb.shape
    samples = cb.shape[2]
    blocks = base // LANES
    stride = 2 * freqs
    wide = 2 * LANES

    def o_copy(m, b):
        slab = o_hbm.at[m].reshape(samples * stride, base).at[:, pl.ds(b * LANES, LANES)]
        return pltpu.make_async_copy(ob.at[m, b], slab, o_sem.at[m, b])

    def c_copy(m):
        return pltpu.make_async_copy(cb.at[m], c_hbm.at[m], c_sem.at[m])

    for m in range(modes):
        gain = s_ref[pl.ds(m, 1), :]
        re, im = (
            (jnp.concatenate([g_ref[2 * m, c], g_ref[2 * m + 1, c]], axis=0).astype(F32) * gain).astype(BF16)
            for c in range(2)
        )
        cb[m, 0] = re
        cb[m, 1] = im
        c_copy(m).start()
        lhs = jnp.concatenate(
            [jnp.concatenate([re, -im], axis=1), jnp.concatenate([im, re], axis=1)], axis=0
        )
        for p in range(blocks // 2):
            for f in range(freqs):
                rhs = jnp.concatenate([eb[m, f, c, p * wide : (p + 1) * wide, :] for c in range(2)], axis=1)
                out = lax.dot_general(lhs, rhs, (((1,), (1,)), ((), ())), preferred_element_type=F32)
                for c in range(2):
                    for i in range(2):
                        of[m, 2 * p + i, pl.ds(2 * f + c, samples, stride=stride), :] = out[
                            c * samples : (c + 1) * samples, i * LANES : (i + 1) * LANES
                        ]
            for b in (2 * p, 2 * p + 1):
                ob[m, b] = of[m, b].astype(BF16)
                o_copy(m, b).start()
    for m in range(modes):
        c_copy(m).wait()
        for b in range(blocks):
            o_copy(m, b).wait()


def per_device(visibilities, eigenmodes, retained):
    modes, samples, freqs, _, base = visibilities.shape
    kmax = eigenmodes.shape[-1]
    blocks = base // LANES
    rows = 2 * samples
    half = samples // 2
    slab = samples * freqs * 2
    group = NX * NY * NCORE
    visibilities, eigenmodes, retained = (
        pltpu.with_memory_space_constraint(a, pltpu.HBM) for a in (visibilities, eigenmodes, retained)
    )
    any_spec = pl.BlockSpec(memory_space=pl.ANY)
    vmem_spec = pl.BlockSpec(memory_space=pltpu.VMEM)
    dma = pltpu.SemaphoreType.DMA
    flops = 2 * modes * rows * freqs * 2 * base * kmax
    gathered, scale, vectors = pl.pallas_call(
        project_kernel,
        out_shape=(
            jax.ShapeDtypeStruct((NY, 2, half, kmax), BF16),
            jax.ShapeDtypeStruct((modes, kmax), F32),
            jax.ShapeDtypeStruct((modes, freqs, 2, base, kmax), BF16),
        ),
        in_specs=[any_spec, any_spec, any_spec],
        out_specs=(vmem_spec, vmem_spec, vmem_spec),
        scratch_shapes=[
            pltpu.SMEM((modes,), jnp.int32),
            pltpu.VMEM((freqs, samples, 2, base), BF16),
            pltpu.VMEM((2, freqs, half, 2, base), BF16),
            pltpu.VMEM((3, kmax // LANES, rows, LANES), F32),
            pltpu.VMEM((3, kmax // LANES, rows, LANES), F32),
            pltpu.VMEM((2, half, kmax), F32),
            pltpu.VMEM((NY - 1, 2, half, kmax), BF16),
            pltpu.VMEM((NY, 2, half, kmax), BF16),
            pltpu.VMEM((NZ, 2 * kmax // LANES, LANES), F32),
            pltpu.VMEM((group, 2 * kmax // LANES, LANES), F32),
            dma,
            dma((freqs,)),
            dma((2, freqs)),
            dma((modes, freqs)),
            dma((NY - 1,)), dma((NY,)),
            dma((NY,)), dma((NY,)),
            dma, dma,
            dma, dma,
        ],
        compiler_params=pltpu.CompilerParams(
            collective_id=0, has_side_effects=True, vmem_limit_bytes=32 << 20
        ),
        cost_estimate=pl.CostEstimate(flops=flops, bytes_accessed=8 << 20, transcendentals=0),
    )(retained, visibilities, eigenmodes)
    coefficients, filtered = pl.pallas_call(
        filter_kernel,
        out_shape=(
            jax.ShapeDtypeStruct((modes, 2, samples, kmax), BF16),
            jax.ShapeDtypeStruct((modes, samples, freqs, 2, base), BF16),
        ),
        in_specs=[vmem_spec, vmem_spec, vmem_spec],
        out_specs=(any_spec, any_spec),
        scratch_shapes=[
            pltpu.VMEM((modes, 2, samples, kmax), BF16),
            pltpu.VMEM((modes, blocks, slab, LANES), F32),
            pltpu.VMEM((modes, blocks, slab, LANES), BF16),
            dma((modes,)),
            dma((modes, blocks)),
        ],
        compiler_params=pltpu.CompilerParams(vmem_limit_bytes=32 << 20),
        cost_estimate=pl.CostEstimate(flops=flops, bytes_accessed=8 << 20, transcendentals=0),
    )(gathered, scale, vectors)
    return coefficients, filtered


def solution(mesh):
    return jax.shard_map(
        per_device,
        mesh=mesh,
        in_specs=(P("ma", None, "freq", None, None), P("ma", "freq", None, None, None), P("ma")),
        out_specs=(P("ma", None, None, None), P("ma", None, "freq", None, None)),
        check_vma=False,
    )
```

```python
import functools

import jax
import jax.numpy as jnp
from jax import lax
from jax.experimental import pallas as pl
from jax.experimental.pallas import tpu as pltpu
from jax.sharding import PartitionSpec as P

MESH = pl.DeviceIdType.MESH
BF16, F32 = jnp.bfloat16, jnp.float32
NX, NZ, NCORE, NY = 4, 8, 2, 4
HUB = 1
LANES = 128


def project_kernel(
    ret_hbm, x_hbm, e_hbm, g_ref, s_ref, eb,
    ret_ref, xb, xh, acc_re, acc_im, pf, sbuf, rbuf, a1, a2,
    ret_sem, x_sem, xh_sem, e_sem, rs_send, rs_recv, ag_send, ag_recv, z_send, z_recv, w_send, w_recv,
):
    modes, freqs, _, base, kmax = eb.shape
    half = pf.shape[1]
    samples = 2 * half
    parts = kmax // LANES
    ma = lax.axis_index("ma")
    y = lax.axis_index("freq")
    core = lax.rem(ma, NCORE)
    z = lax.rem(ma // NCORE, NZ)
    x = ma // (NCORE * NZ)

    mine = lax.rem(y, 2)
    first, second = 1 - y // 2, y // 2

    def x_copy(f):
        return pltpu.make_async_copy(x_hbm.at[first, :, f], xb.at[f], x_sem.at[f])

    def xh_copy(own, f):
        start = pl.multiple_of((mine if own else 1 - mine) * half, half)
        return pltpu.make_async_copy(x_hbm.at[second, pl.ds(start, half), f], xh.at[own, f], xh_sem.at[own, f])

    def e_copy(m, f):
        return pltpu.make_async_copy(e_hbm.at[m, f], eb.at[m, f], e_sem.at[m, f])

    for f in range(freqs):
        x_copy(f).start()
        e_copy(first, f).start()
    for f in range(freqs):
        xh_copy(0, f).start()
        e_copy(second, f).start()
    for f in range(freqs):
        xh_copy(1, f).start()
    ret_copy = pltpu.make_async_copy(ret_hbm, ret_ref, ret_sem)
    ret_copy.start()

    zs = [lax.rem(z + d, NZ) for d in range(NZ)]
    xs = [lax.rem(x + d, NX) for d in range(NX)]
    ys = [lax.rem(y + d, NY) for d in range(NY)]
    far = [2, 1, 3, 0]
    flat = [(dx, dy) for dx in far for dy in far]

    def on_z(d, c):
        return {"ma": (x * NZ + zs[d]) * NCORE + c, "freq": y}

    def on_xy(dx, dy, c):
        return {"ma": (xs[dx] * NZ + z) * NCORE + c, "freq": ys[dy]}

    barrier = pltpu.get_barrier_semaphore()

    def greet(peer):
        pl.semaphore_signal(barrier, inc=1, device_id=peer, device_id_type=MESH)

    for dx, dy in flat:
        greet(on_xy(dx, dy, 1 - core))
    for d in range(1, NZ):
        greet(on_z(d, 1 - core))
    for d in range(1, NY):
        greet(on_xy(0, d, core))

    @pl.when(core == HUB)
    def _():
        for dx, dy in flat:
            if dx:
                greet(on_xy(dx, dy, core))
        for d in range(1, NZ):
            greet(on_z(d, core))

    greeted = NX * NY + (NZ - 1) + (NY - 1)
    is_hub = core if HUB == 1 else 1 - core
    greeted = greeted + is_hub * ((NX - 1) * NY + NZ - 1)

    def rs_copy(i, part, t):
        return pltpu.make_async_remote_copy(
            src_ref=sbuf.at[part], dst_ref=rbuf.at[y], send_sem=rs_send.at[i], recv_sem=rs_recv.at[y],
            device_id={"ma": ma, "freq": t}, device_id_type=MESH,
        )

    rs_copies = (
        rs_copy(0, mine, 2 * first + mine),
        rs_copy(1, 1 - mine, 2 * first + 1 - mine),
        rs_copy(2, 2, 2 * second + 1 - mine),
    )

    def project(unit, m, f, lhs):
        count = lhs.shape[0]
        for c, acc in ((0, acc_re), (1, acc_im)):
            d = jnp.dot(lhs, eb[m, f, c], preferred_element_type=F32)
            for p in range(parts):
                piece = d[:, p * LANES : (p + 1) * LANES]
                acc[unit, p, :count] = piece if f == 0 else acc[unit, p, :count] + piece

    def combine(unit, count, put):
        even, odd = pl.ds(0, count, stride=2), pl.ds(1, count, stride=2)
        for p in range(parts):
            lanes = slice(p * LANES, (p + 1) * LANES)
            put(0, lanes, acc_re[unit, p, even, :] + acc_im[unit, p, odd, :])
            put(1, lanes, acc_re[unit, p, odd, :] - acc_im[unit, p, even, :])

    def put_halves(c, lanes, value):
        for h in range(2):
            sbuf[h, c, :, lanes] = value[h * half : (h + 1) * half].astype(BF16)

    def put_partner(c, lanes, value):
        sbuf[2, c, :, lanes] = value.astype(BF16)

    def put_own(c, lanes, value):
        pf[c, :, lanes] = value

    for f in range(freqs):
        x_copy(f).wait()
        e_copy(first, f).wait()
        project(0, first, f, xb[f].reshape(2 * samples, base))
    combine(0, samples, put_halves)
    pl.semaphore_wait(barrier, greeted)
    rs_copies[0].start()
    rs_copies[1].start()
    for f in range(freqs):
        xh_copy(0, f).wait()
        e_copy(second, f).wait()
        project(1, second, f, xh[0, f].reshape(samples, base))
    combine(1, half, put_partner)
    rs_copies[2].start()
    for f in range(freqs):
        xh_copy(1, f).wait()
        project(2, second, f, xh[1, f].reshape(samples, base))
    combine(2, half, put_own)
    share = pf[...]
    for d in range(1, NY):
        src = ys[d]
        pltpu.make_async_remote_copy(
            src_ref=sbuf.at[0], dst_ref=rbuf.at[src],
            send_sem=rs_send.at[d - 1], recv_sem=rs_recv.at[src],
            device_id={"ma": ma, "freq": src}, device_id_type=MESH,
        ).wait_recv()
        share = share + rbuf[src].astype(F32)
    ret_copy.wait()
    ranks = lax.broadcasted_iota(jnp.int32, (1, kmax), 1)
    keep = (ranks < ret_ref[y // 2]).astype(F32)
    power = keep * jnp.sum(share[0] * share[0] + share[1] * share[1], axis=0, keepdims=True)
    count = keep * half
    spot = z * NCORE + core
    for p in range(parts):
        a1[spot, pl.ds(p, 1), :] = power[:, p * LANES : (p + 1) * LANES]
        a1[spot, pl.ds(parts + p, 1), :] = count[:, p * LANES : (p + 1) * LANES]

    def z_copy(d):
        return pltpu.make_async_remote_copy(
            src_ref=a1.at[spot], dst_ref=a1.at[spot], send_sem=z_send, recv_sem=z_recv,
            device_id=on_z(d, HUB), device_id_type=MESH,
        )

    for d in (4, 3, 5, 2, 6, 1, 7):
        z_copy(d).start()

    @pl.when(core != HUB)
    def _():
        z_copy(0).start()

    g_ref[y] = share.astype(BF16)

    def ag_copy(d):
        return pltpu.make_async_remote_copy(
            src_ref=g_ref.at[y], dst_ref=g_ref.at[y], send_sem=ag_send.at[d], recv_sem=ag_recv.at[y],
            device_id={"ma": ma, "freq": ys[d]}, device_id_type=MESH,
        )

    for d in (2, 1, 3):
        ag_copy(d).start()

    def settle(ref, count, sem):
        pltpu.make_async_copy(ref.at[pl.ds(0, count)], ref.at[pl.ds(0, count)], sem).wait()

    q = x * NY + y

    @pl.when(core == HUB)
    def _():
        settle(a1, NZ * NCORE - 1, z_recv)
        total = a1[0]
        for i in range(1, NZ * NCORE):
            total = total + a1[i]
        a2[q] = total
        for dx, dy in flat:
            for c in (1 - HUB, HUB):
                if (dx, dy, c) != (0, 0, HUB):
                    pltpu.make_async_remote_copy(
                        src_ref=a2.at[q], dst_ref=a2.at[q], send_sem=w_send, recv_sem=w_recv,
                        device_id=on_xy(dx, dy, c), device_id_type=MESH,
                    ).start()
        settle(a2, NX * NY - 1, w_recv)

    @pl.when(core != HUB)
    def _():
        settle(a2, NX * NY, w_recv)

    total = a2[0]
    for i in range(1, NX * NY):
        total = total + a2[i]
    scale = 1.0 / jnp.sqrt(total[:parts] / jnp.maximum(total[parts:], 1.0) + 1e-06)
    scale = jnp.concatenate([scale[p : p + 1, :] for p in range(parts)], axis=1)
    for m in range(modes):
        s_ref[pl.ds(m, 1), :] = (ranks < ret_ref[m]).astype(F32) * scale

    for d in range(1, NY):
        src = ys[d]
        pltpu.make_async_remote_copy(
            src_ref=g_ref.at[y], dst_ref=g_ref.at[src], send_sem=ag_send.at[d], recv_sem=ag_recv.at[src],
            device_id={"ma": ma, "freq": src}, device_id_type=MESH,
        ).wait_recv()
    for copy in rs_copies:
        copy.wait_send()
    for d in range(1, NY):
        ag_copy(d).wait_send()
    @pl.when(core == HUB)
    def _():
        settle(a1, NZ - 1, z_send)
        settle(a2, NX * NY * NCORE - 1, w_send)

    @pl.when(core != HUB)
    def _():
        settle(a1, NZ, z_send)


def filter_kernel(g_ref, s_ref, eb, c_hbm, o_hbm, cb, of, ob, c_sem, o_sem):
    modes, freqs, _, base, kmax = eb.shape
    samples = cb.shape[2]
    blocks = base // LANES
    stride = 2 * freqs
    wide = 2 * LANES

    def o_copy(m, b):
        slab = o_hbm.at[m].reshape(samples * stride, base).at[:, pl.ds(b * LANES, LANES)]
        return pltpu.make_async_copy(ob.at[m, b], slab, o_sem.at[m, b])

    def c_copy(m):
        return pltpu.make_async_copy(cb.at[m], c_hbm.at[m], c_sem.at[m])

    for m in range(modes):
        gain = s_ref[pl.ds(m, 1), :]
        re, im = (
            (jnp.concatenate([g_ref[2 * m, c], g_ref[2 * m + 1, c]], axis=0).astype(F32) * gain).astype(BF16)
            for c in range(2)
        )
        cb[m, 0] = re
        cb[m, 1] = im
        c_copy(m).start()
        lhs = jnp.concatenate(
            [jnp.concatenate([re, -im], axis=1), jnp.concatenate([im, re], axis=1)], axis=0
        )
        for p in range(blocks // 2):
            for f in range(freqs):
                rhs = jnp.concatenate([eb[m, f, c, p * wide : (p + 1) * wide, :] for c in range(2)], axis=1)
                out = lax.dot_general(lhs, rhs, (((1,), (1,)), ((), ())), preferred_element_type=F32)
                for c in range(2):
                    for i in range(2):
                        of[m, 2 * p + i, pl.ds(2 * f + c, samples, stride=stride), :] = out[
                            c * samples : (c + 1) * samples, i * LANES : (i + 1) * LANES
                        ]
            for b in (2 * p, 2 * p + 1):
                ob[m, b] = of[m, b].astype(BF16)
                o_copy(m, b).start()
    for m in range(modes):
        c_copy(m).wait()
        for b in range(blocks):
            o_copy(m, b).wait()


def per_device(visibilities, eigenmodes, retained):
    modes, samples, freqs, _, base = visibilities.shape
    kmax = eigenmodes.shape[-1]
    blocks = base // LANES
    rows = 2 * samples
    half = samples // 2
    slab = samples * freqs * 2
    visibilities, eigenmodes, retained = (
        pltpu.with_memory_space_constraint(a, pltpu.HBM) for a in (visibilities, eigenmodes, retained)
    )
    any_spec = pl.BlockSpec(memory_space=pl.ANY)
    vmem_spec = pl.BlockSpec(memory_space=pltpu.VMEM)
    dma = pltpu.SemaphoreType.DMA
    flops = 2 * modes * rows * freqs * 2 * base * kmax
    gathered, scale, vectors = pl.pallas_call(
        project_kernel,
        out_shape=(
            jax.ShapeDtypeStruct((NY, 2, half, kmax), BF16),
            jax.ShapeDtypeStruct((modes, kmax), F32),
            jax.ShapeDtypeStruct((modes, freqs, 2, base, kmax), BF16),
        ),
        in_specs=[any_spec, any_spec, any_spec],
        out_specs=(vmem_spec, vmem_spec, vmem_spec),
        scratch_shapes=[
            pltpu.SMEM((modes,), jnp.int32),
            pltpu.VMEM((freqs, samples, 2, base), BF16),
            pltpu.VMEM((2, freqs, half, 2, base), BF16),
            pltpu.VMEM((3, kmax // LANES, rows, LANES), F32),
            pltpu.VMEM((3, kmax // LANES, rows, LANES), F32),
            pltpu.VMEM((2, half, kmax), F32),
            pltpu.VMEM((NY - 1, 2, half, kmax), BF16),
            pltpu.VMEM((NY, 2, half, kmax), BF16),
            pltpu.VMEM((NZ * NCORE, 2 * kmax // LANES, LANES), F32),
            pltpu.VMEM((NX * NY * NCORE, 2 * kmax // LANES, LANES), F32),
            dma,
            dma((freqs,)),
            dma((2, freqs)),
            dma((modes, freqs)),
            dma((NY - 1,)), dma((NY,)),
            dma((NY,)), dma((NY,)),
            dma, dma,
            dma, dma,
        ],
        compiler_params=pltpu.CompilerParams(
            collective_id=0, has_side_effects=True, vmem_limit_bytes=32 << 20
        ),
        cost_estimate=pl.CostEstimate(flops=flops, bytes_accessed=8 << 20, transcendentals=0),
    )(retained, visibilities, eigenmodes)
    coefficients, filtered = pl.pallas_call(
        filter_kernel,
        out_shape=(
            jax.ShapeDtypeStruct((modes, 2, samples, kmax), BF16),
            jax.ShapeDtypeStruct((modes, samples, freqs, 2, base), BF16),
        ),
        in_specs=[vmem_spec, vmem_spec, vmem_spec],
        out_specs=(any_spec, any_spec),
        scratch_shapes=[
            pltpu.VMEM((modes, 2, samples, kmax), BF16),
            pltpu.VMEM((modes, blocks, slab, LANES), F32),
            pltpu.VMEM((modes, blocks, slab, LANES), BF16),
            dma((modes,)),
            dma((modes, blocks)),
        ],
        compiler_params=pltpu.CompilerParams(vmem_limit_bytes=32 << 20),
        cost_estimate=pl.CostEstimate(flops=flops, bytes_accessed=8 << 20, transcendentals=0),
    )(gathered, scale, vectors)
    return coefficients, filtered


def solution(mesh):
    return jax.shard_map(
        per_device,
        mesh=mesh,
        in_specs=(P("ma", None, "freq", None, None), P("ma", "freq", None, None, None), P("ma")),
        out_specs=(P("ma", None, None, None), P("ma", None, "freq", None, None)),
        check_vma=False,
    )
```

```python
import functools

import jax
import jax.numpy as jnp
from jax import lax
from jax.experimental import pallas as pl
from jax.experimental.pallas import tpu as pltpu
from jax.sharding import PartitionSpec as P

MESH = pl.DeviceIdType.MESH
BF16, F32 = jnp.bfloat16, jnp.float32
NX, NZ, NCORE, NY = 4, 8, 2, 4
HUB = 1
LANES = 128


def added(terms):
    while len(terms) > 1:
        terms = [a + b for a, b in zip(terms[::2], terms[1::2])]
    return terms[0]


def project_kernel(
    ret_hbm, x_hbm, e_hbm, g_ref, s_ref, eb,
    ret_ref, xb, xh, acc_re, acc_im, pf, sbuf, rbuf, a1, a2,
    ret_sem, x_sem, xh_sem, e_sem, rs_send, rs_recv, ag_send, ag_recv, z_send, z_recv, w_send, w_recv,
):
    modes, freqs, _, base, kmax = eb.shape
    half = pf.shape[1]
    samples = 2 * half
    parts = kmax // LANES
    ma = lax.axis_index("ma")
    y = lax.axis_index("freq")
    core = lax.rem(ma, NCORE)
    z = lax.rem(ma // NCORE, NZ)
    x = ma // (NCORE * NZ)

    mine = lax.rem(y, 2)
    first, second = 1 - y // 2, y // 2

    def x_copy(f):
        return pltpu.make_async_copy(x_hbm.at[first, :, f], xb.at[f], x_sem.at[f])

    def xh_copy(own, f):
        start = pl.multiple_of((mine if own else 1 - mine) * half, half)
        return pltpu.make_async_copy(x_hbm.at[second, pl.ds(start, half), f], xh.at[own, f], xh_sem.at[own, f])

    def e_copy(m, f):
        return pltpu.make_async_copy(e_hbm.at[m, f], eb.at[m, f], e_sem.at[m, f])

    for f in range(freqs):
        x_copy(f).start()
        e_copy(first, f).start()
    for f in range(freqs):
        xh_copy(0, f).start()
        e_copy(second, f).start()
    for f in range(freqs):
        xh_copy(1, f).start()
    ret_copy = pltpu.make_async_copy(ret_hbm, ret_ref, ret_sem)
    ret_copy.start()

    zs = [lax.rem(z + d, NZ) for d in range(NZ)]
    xs = [lax.rem(x + d, NX) for d in range(NX)]
    ys = [lax.rem(y + d, NY) for d in range(NY)]
    far = [2, 1, 3, 0]
    flat = [(dx, dy) for dx in far for dy in far]

    def on_z(d, c):
        return {"ma": (x * NZ + zs[d]) * NCORE + c, "freq": y}

    def on_xy(dx, dy, c):
        return {"ma": (xs[dx] * NZ + z) * NCORE + c, "freq": ys[dy]}

    barrier = pltpu.get_barrier_semaphore()

    def greet(peer):
        pl.semaphore_signal(barrier, inc=1, device_id=peer, device_id_type=MESH)

    for dx, dy in flat:
        greet(on_xy(dx, dy, 1 - core))
    for d in range(1, NZ):
        greet(on_z(d, 1 - core))
    for d in range(1, NY):
        greet(on_xy(0, d, core))

    @pl.when(core == HUB)
    def _():
        for dx, dy in flat:
            if dx:
                greet(on_xy(dx, dy, core))
        for d in range(1, NZ):
            greet(on_z(d, core))

    greeted = NX * NY + (NZ - 1) + (NY - 1)
    is_hub = core if HUB == 1 else 1 - core
    greeted = greeted + is_hub * ((NX - 1) * NY + NZ - 1)

    def rs_copy(i, part, t):
        return pltpu.make_async_remote_copy(
            src_ref=sbuf.at[part], dst_ref=rbuf.at[y], send_sem=rs_send.at[i], recv_sem=rs_recv.at[y],
            device_id={"ma": ma, "freq": t}, device_id_type=MESH,
        )

    rs_copies = (
        rs_copy(0, mine, 2 * first + mine),
        rs_copy(1, 1 - mine, 2 * first + 1 - mine),
        rs_copy(2, 2, 2 * second + 1 - mine),
    )

    def project(unit, m, f, lhs):
        count = lhs.shape[0]
        for c, acc in ((0, acc_re), (1, acc_im)):
            d = jnp.dot(lhs, eb[m, f, c], preferred_element_type=F32)
            for p in range(parts):
                piece = d[:, p * LANES : (p + 1) * LANES]
                acc[unit, p, :count] = piece if f == 0 else acc[unit, p, :count] + piece

    def combine(unit, count, put):
        even, odd = pl.ds(0, count, stride=2), pl.ds(1, count, stride=2)
        for p in range(parts):
            lanes = slice(p * LANES, (p + 1) * LANES)
            put(0, lanes, acc_re[unit, p, even, :] + acc_im[unit, p, odd, :])
            put(1, lanes, acc_re[unit, p, odd, :] - acc_im[unit, p, even, :])

    def put_halves(c, lanes, value):
        for h in range(2):
            sbuf[h, c, :, lanes] = value[h * half : (h + 1) * half].astype(BF16)

    def put_partner(c, lanes, value):
        sbuf[2, c, :, lanes] = value.astype(BF16)

    def put_own(c, lanes, value):
        pf[c, :, lanes] = value

    for f in range(freqs):
        x_copy(f).wait()
        e_copy(first, f).wait()
        project(0, first, f, xb[f].reshape(2 * samples, base))
    combine(0, samples, put_halves)
    pl.semaphore_wait(barrier, greeted)
    rs_copies[0].start()
    rs_copies[1].start()
    for f in range(freqs):
        xh_copy(0, f).wait()
        e_copy(second, f).wait()
        project(1, second, f, xh[0, f].reshape(samples, base))
    combine(1, half, put_partner)
    rs_copies[2].start()
    for f in range(freqs):
        xh_copy(1, f).wait()
        project(2, second, f, xh[1, f].reshape(samples, base))
    combine(2, half, put_own)
    share = pf[...]
    for d, src in ((1, 2 * first + mine), (2, 2 * first + 1 - mine), (3, 2 * second + 1 - mine)):
        pltpu.make_async_remote_copy(
            src_ref=sbuf.at[0], dst_ref=rbuf.at[src],
            send_sem=rs_send.at[d - 1], recv_sem=rs_recv.at[src],
            device_id={"ma": ma, "freq": src}, device_id_type=MESH,
        ).wait_recv()
        share = share + rbuf[src].astype(F32)
    ret_copy.wait()
    ranks = lax.broadcasted_iota(jnp.int32, (1, kmax), 1)
    keep = (ranks < ret_ref[y // 2]).astype(F32)
    power = keep * jnp.sum(share[0] * share[0] + share[1] * share[1], axis=0, keepdims=True)
    count = keep * half
    spot = z * NCORE + core
    for p in range(parts):
        a1[spot, pl.ds(p, 1), :] = power[:, p * LANES : (p + 1) * LANES]
        a1[spot, pl.ds(parts + p, 1), :] = count[:, p * LANES : (p + 1) * LANES]

    def z_copy(d):
        return pltpu.make_async_remote_copy(
            src_ref=a1.at[spot], dst_ref=a1.at[spot], send_sem=z_send, recv_sem=z_recv,
            device_id=on_z(d, HUB), device_id_type=MESH,
        )

    for d in (4, 3, 5, 2, 6, 1, 7):
        z_copy(d).start()

    @pl.when(core != HUB)
    def _():
        z_copy(0).start()

    g_ref[y] = share.astype(BF16)

    def ag_copy(d):
        return pltpu.make_async_remote_copy(
            src_ref=g_ref.at[y], dst_ref=g_ref.at[y], send_sem=ag_send.at[d], recv_sem=ag_recv.at[y],
            device_id={"ma": ma, "freq": ys[d]}, device_id_type=MESH,
        )

    for d in (2, 1, 3):
        ag_copy(d).start()

    def settle(ref, count, sem):
        pltpu.make_async_copy(ref.at[pl.ds(0, count)], ref.at[pl.ds(0, count)], sem).wait()

    q = x * NY + y

    @pl.when(core == HUB)
    def _():
        settle(a1, NZ * NCORE - 1, z_recv)
        total = added([a1[i] for i in range(NZ * NCORE)])
        a2[q] = total
        for dx, dy in flat:
            for c in (1 - HUB, HUB):
                if (dx, dy, c) != (0, 0, HUB):
                    pltpu.make_async_remote_copy(
                        src_ref=a2.at[q], dst_ref=a2.at[q], send_sem=w_send, recv_sem=w_recv,
                        device_id=on_xy(dx, dy, c), device_id_type=MESH,
                    ).start()
        settle(a2, NX * NY - 1, w_recv)

    @pl.when(core != HUB)
    def _():
        settle(a2, NX * NY, w_recv)

    total = added([a2[i] for i in range(NX * NY)])
    scale = 1.0 / jnp.sqrt(total[:parts] / jnp.maximum(total[parts:], 1.0) + 1e-06)
    scale = jnp.concatenate([scale[p : p + 1, :] for p in range(parts)], axis=1)
    for m in range(modes):
        s_ref[pl.ds(m, 1), :] = (ranks < ret_ref[m]).astype(F32) * scale

    for d in range(1, NY):
        src = ys[d]
        pltpu.make_async_remote_copy(
            src_ref=g_ref.at[y], dst_ref=g_ref.at[src], send_sem=ag_send.at[d], recv_sem=ag_recv.at[src],
            device_id={"ma": ma, "freq": src}, device_id_type=MESH,
        ).wait_recv()
    for copy in rs_copies:
        copy.wait_send()
    for d in range(1, NY):
        ag_copy(d).wait_send()
    @pl.when(core == HUB)
    def _():
        settle(a1, NZ - 1, z_send)
        settle(a2, NX * NY * NCORE - 1, w_send)

    @pl.when(core != HUB)
    def _():
        settle(a1, NZ, z_send)


def filter_kernel(g_ref, s_ref, eb, c_hbm, o_hbm, cb, of, ob, c_sem, o_sem):
    modes, freqs, _, base, kmax = eb.shape
    samples = cb.shape[2]
    blocks = base // LANES
    stride = 2 * freqs
    wide = 2 * LANES

    def o_copy(m, b):
        slab = o_hbm.at[m].reshape(samples * stride, base).at[:, pl.ds(b * LANES, LANES)]
        return pltpu.make_async_copy(ob.at[m, b], slab, o_sem.at[m, b])

    def c_copy(m):
        return pltpu.make_async_copy(cb.at[m], c_hbm.at[m], c_sem.at[m])

    for m in range(modes):
        gain = s_ref[pl.ds(m, 1), :]
        re, im = (
            (jnp.concatenate([g_ref[2 * m, c], g_ref[2 * m + 1, c]], axis=0).astype(F32) * gain).astype(BF16)
            for c in range(2)
        )
        cb[m, 0] = re
        cb[m, 1] = im
        c_copy(m).start()
        lhs = jnp.concatenate(
            [jnp.concatenate([re, -im], axis=1), jnp.concatenate([im, re], axis=1)], axis=0
        )
        for p in range(blocks // 2):
            for f in range(freqs):
                rhs = jnp.concatenate([eb[m, f, c, p * wide : (p + 1) * wide, :] for c in range(2)], axis=1)
                out = lax.dot_general(lhs, rhs, (((1,), (1,)), ((), ())), preferred_element_type=F32)
                for c in range(2):
                    for i in range(2):
                        of[m, 2 * p + i, pl.ds(2 * f + c, samples, stride=stride), :] = out[
                            c * samples : (c + 1) * samples, i * LANES : (i + 1) * LANES
                        ]
            for b in (2 * p, 2 * p + 1):
                ob[m, b] = of[m, b].astype(BF16)
                o_copy(m, b).start()
    for m in range(modes):
        c_copy(m).wait()
        for b in range(blocks):
            o_copy(m, b).wait()


def per_device(visibilities, eigenmodes, retained):
    modes, samples, freqs, _, base = visibilities.shape
    kmax = eigenmodes.shape[-1]
    blocks = base // LANES
    rows = 2 * samples
    half = samples // 2
    slab = samples * freqs * 2
    visibilities, eigenmodes, retained = (
        pltpu.with_memory_space_constraint(a, pltpu.HBM) for a in (visibilities, eigenmodes, retained)
    )
    any_spec = pl.BlockSpec(memory_space=pl.ANY)
    vmem_spec = pl.BlockSpec(memory_space=pltpu.VMEM)
    dma = pltpu.SemaphoreType.DMA
    flops = 2 * modes * rows * freqs * 2 * base * kmax
    gathered, scale, vectors = pl.pallas_call(
        project_kernel,
        out_shape=(
            jax.ShapeDtypeStruct((NY, 2, half, kmax), BF16),
            jax.ShapeDtypeStruct((modes, kmax), F32),
            jax.ShapeDtypeStruct((modes, freqs, 2, base, kmax), BF16),
        ),
        in_specs=[any_spec, any_spec, any_spec],
        out_specs=(vmem_spec, vmem_spec, vmem_spec),
        scratch_shapes=[
            pltpu.SMEM((modes,), jnp.int32),
            pltpu.VMEM((freqs, samples, 2, base), BF16),
            pltpu.VMEM((2, freqs, half, 2, base), BF16),
            pltpu.VMEM((3, kmax // LANES, rows, LANES), F32),
            pltpu.VMEM((3, kmax // LANES, rows, LANES), F32),
            pltpu.VMEM((2, half, kmax), F32),
            pltpu.VMEM((NY - 1, 2, half, kmax), BF16),
            pltpu.VMEM((NY, 2, half, kmax), BF16),
            pltpu.VMEM((NZ * NCORE, 2 * kmax // LANES, LANES), F32),
            pltpu.VMEM((NX * NY * NCORE, 2 * kmax // LANES, LANES), F32),
            dma,
            dma((freqs,)),
            dma((2, freqs)),
            dma((modes, freqs)),
            dma((NY - 1,)), dma((NY,)),
            dma((NY,)), dma((NY,)),
            dma, dma,
            dma, dma,
        ],
        compiler_params=pltpu.CompilerParams(
            collective_id=0, has_side_effects=True, vmem_limit_bytes=32 << 20
        ),
        cost_estimate=pl.CostEstimate(flops=flops, bytes_accessed=8 << 20, transcendentals=0),
    )(retained, visibilities, eigenmodes)
    coefficients, filtered = pl.pallas_call(
        filter_kernel,
        out_shape=(
            jax.ShapeDtypeStruct((modes, 2, samples, kmax), BF16),
            jax.ShapeDtypeStruct((modes, samples, freqs, 2, base), BF16),
        ),
        in_specs=[vmem_spec, vmem_spec, vmem_spec],
        out_specs=(any_spec, any_spec),
        scratch_shapes=[
            pltpu.VMEM((modes, 2, samples, kmax), BF16),
            pltpu.VMEM((modes, blocks, slab, LANES), F32),
            pltpu.VMEM((modes, blocks, slab, LANES), BF16),
            dma((modes,)),
            dma((modes, blocks)),
        ],
        compiler_params=pltpu.CompilerParams(vmem_limit_bytes=32 << 20),
        cost_estimate=pl.CostEstimate(flops=flops, bytes_accessed=8 << 20, transcendentals=0),
    )(gathered, scale, vectors)
    return coefficients, filtered


def solution(mesh):
    return jax.shard_map(
        per_device,
        mesh=mesh,
        in_specs=(P("ma", None, "freq", None, None), P("ma", "freq", None, None, None), P("ma")),
        out_specs=(P("ma", None, None, None), P("ma", None, "freq", None, None)),
        check_vma=False,
    )
```
